128 devices in a mesh: row: 16 (over y_hi, x, core), col: 8 (over z, y_lo).
Axes of the slice: x: 4, y: 4 (y_hi: 2, y_lo: 2; y = y_hi * 2 + y_lo), z: 4, core: 2. Of those that a mesh axis runs over, the one named last changes fastest.
Arguments:
- residual: bfloat16 [16, 8, 2048, 512], P('row', 'col'), may hold values from -6 to 6
- self_tiles: bfloat16 [16, 8, 2048, 2048], P('row', 'col'), may hold values from -0.09375 to 0.09375
- side_tiles: bfloat16 [16, 8, 2048, 2048], P('row', 'col'), may hold values from -0.09375 to 0.09375
- row_cluster_basis: bfloat16 [16, 8, 2048, 32], P('row', 'col'), may hold values from -0.125 to 0.125
- column_cluster_basis: bfloat16 [16, 8, 2048, 32], P('row', 'col'), may hold values from -1 to 1
- couplings: bfloat16 [16, 8, 64, 32, 32], P('row', 'col'), may hold values from -0.1875 to 0.1875
- near_side: int32 [16, 8], P('row', 'col'), may hold values from -1 to 1
- adm_targets: int32 [16, 8, 64], P('row', 'col'), may hold values from 0 to 127, as said below
- adm_ranks: int32 [16, 8, 64], P('row', 'col'), may hold values from 8 to 32
- adm_count: int32 [16, 8], P('row', 'col'), may hold values from 1 to 64
Outputs:
- gradient: float32 [16, 8, 2048, 512], P('row', 'col')
The draws below stay inside these ranges and needn't reach their ends.
Inputs may be any that keep to these rules, and one draw needn't show every extreme that they name: `near_side`: -1 or +1 names the cluster row before or after around the loop of 16 rows; 0 means no such tile. Each entry of adm_targets for the block row of linear index i is the linear index of a cluster other than i; slot 0 names i - 1 or i + 1, counted round the 128 clusters; targets may repeat.
All inputs are finite; a program needn't handle non-finite values.
Results may differ from the reference program's by a relative error of at most 0.0033.
Values may be sent and summed in bfloat16 or wider, within the bound.
A program may use at most 128 MiB of HBM per device.

```python
import jax
import jax.numpy as jnp
from jax import lax

LEAF = 2048
K = 32
NRHS = 512
ADM = 64
GRID_R = 16
GRID_C = 8


def draw_adm_targets(key, part):
    base = jax.random.fold_in(key, 11)
    first_key, second_key = jax.random.split(base)
    total = GRID_R * GRID_C
    linear = (jnp.arange(GRID_R, dtype=jnp.int32)[:, None] * GRID_C + jnp.arange(GRID_C, dtype=jnp.int32)[None, :])[:, :, None]
    offsets = jax.random.randint(first_key, (GRID_R, GRID_C, ADM), 1, total, dtype=jnp.int32)
    signs = jax.random.randint(second_key, (GRID_R, GRID_C, 1), 0, 2, dtype=jnp.int32) * 2 - 1
    slot_index = jnp.arange(ADM, dtype=jnp.int32)[None, None, :]
    chosen = jnp.where(slot_index == 0, signs + total, offsets)
    return ((linear + chosen) % total).astype(jnp.int32)


def plant(values, key, least, largest):
    shape = values.shape
    index_at = [jax.random.randint(jax.random.fold_in(key, axis), (), 0, shape[axis]) for axis in range(len(shape))]
    values = values.at[tuple(index_at)].set(least)
    longest = shape.index(max(shape))
    index_at[longest] = (index_at[longest] + 1) % shape[longest]
    return values.at[tuple(index_at)].set(largest)


def levels(stream_key, shape, cuts, least, high):
    factor_of = 1.0
    for dim, blocks in cuts:
        heights = jax.random.uniform(jax.random.fold_in(jax.random.fold_in(stream_key, 6), dim), (blocks,), jnp.float32, least / len(cuts), high / len(cuts))
        factor_of = factor_of * jnp.repeat(jnp.exp(heights), shape[dim] // blocks).reshape((-1,) + (1,) * (len(shape) - 1 - dim))
    return factor_of


def centred(stream_key, shape, width, limit, pieces=(), held_as=jnp.bfloat16):
    level = levels(stream_key, shape, pieces, -0.22, 0.18) if pieces else 1.0
    values = jax.random.normal(stream_key, shape, jnp.float32) * width * level
    return jnp.minimum(jnp.maximum(values, -limit), limit).astype(held_as)


def setup_inputs(seed: int = 0) -> dict:
    key_of = jax.random.split(jax.random.key(seed), 11)
    return {
        "residual": centred(key_of[0], (GRID_R, GRID_C, LEAF, NRHS), 1.0, 6.0, ((0, 16), (1, 8))),
        "self_tiles": centred(key_of[1], (GRID_R, GRID_C, LEAF, LEAF), (2 * LEAF) ** -0.5, 0.09375, ((0, 16), (1, 8))),
        "side_tiles": centred(key_of[2], (GRID_R, GRID_C, LEAF, LEAF), (2 * LEAF) ** -0.5, 0.09375, ((0, 16), (1, 8))),
        "row_cluster_basis": centred(key_of[3], (GRID_R, GRID_C, LEAF, K), LEAF ** -0.5, 0.125, ((0, 16), (1, 8))),
        "column_cluster_basis": centred(key_of[4], (GRID_R, GRID_C, LEAF, K), K ** -0.5, 1.0, ((0, 16), (1, 8))),
        "couplings": centred(key_of[5], (GRID_R, GRID_C, ADM, K, K), (K * ADM // 2) ** -0.5, 0.1875, ((0, 16), (1, 8))),
        "near_side": plant(jax.random.randint(key_of[6], (GRID_R, GRID_C), -1, 2), jax.random.fold_in(key_of[6], 1), -1, 1).astype(jnp.int32),
        "adm_targets": draw_adm_targets(jax.random.fold_in(key_of[10], 71), 0),
        "adm_ranks": plant(jax.random.randint(key_of[8], (GRID_R, GRID_C, ADM), K // 4, K + 1), jax.random.fold_in(key_of[8], 1), K // 4, K).astype(jnp.int32),
        "adm_count": plant(jax.random.randint(key_of[9], (GRID_R, GRID_C), 1, ADM + 1), jax.random.fold_in(key_of[9], 1), 1, ADM).astype(jnp.int32),
    }


def reference(residual, self_tiles, side_tiles, row_cluster_basis, column_cluster_basis, couplings, near_side, adm_targets, adm_ranks, adm_count):
    grid_rows, grid_cols, sample_points, columns = residual.shape
    slot_count = couplings.shape[2]
    rank_dimension = couplings.shape[3]
    cluster_groups = grid_rows * grid_cols
    flattened_result = residual.reshape(cluster_groups, sample_points, columns)
    coefficient_table = jnp.einsum("qhs,qhe->qse", row_cluster_basis.reshape(cluster_groups, sample_points, rank_dimension).astype(jnp.float32), flattened_result.astype(jnp.float32), precision=lax.Precision.HIGHEST).astype(jnp.bfloat16)
    rank_index = jnp.arange(rank_dimension, dtype=jnp.int32)
    slot_index = jnp.arange(slot_count, dtype=jnp.int32)
    keep_mask = (rank_index[None, None, None, :] < adm_ranks[:, :, :, None]) & (slot_index[None, None, :, None] < adm_count[:, :, None, None])
    keep_float = keep_mask.astype(jnp.float32)
    masked = couplings.astype(jnp.float32) * keep_float[:, :, :, :, None] * keep_float[:, :, :, None, :]
    masked = masked.reshape(cluster_groups, slot_count, rank_dimension, rank_dimension)
    targets = adm_targets.reshape(cluster_groups, slot_count).astype(jnp.int32)

    def add_row(running, inputs):
        block, coeff_block, target_row = inputs
        contrib = jnp.einsum("sab,an->sbn", block, coeff_block.astype(jnp.float32), precision=lax.Precision.HIGHEST)
        return running.at[target_row].add(contrib), jnp.zeros((), jnp.float32)

    result = lax.scan(add_row, jnp.zeros((cluster_groups, rank_dimension, columns), jnp.float32), (masked, coefficient_table, targets))
    dual_vector = result[0].astype(jnp.bfloat16)
    distant_part = jnp.einsum("qpo,qou->qpu", column_cluster_basis.reshape(cluster_groups, sample_points, rank_dimension).astype(jnp.float32), dual_vector.astype(jnp.float32), precision=lax.Precision.HIGHEST)
    from_above = jnp.roll(residual, 1, axis=0)
    from_below = jnp.roll(residual, -1, axis=0)
    side_offset = near_side[:, :, None, None]
    neighbour = jnp.where(side_offset == -1, from_above, jnp.where(side_offset == 1, from_below, jnp.zeros_like(residual)))

    def near_block(inputs):
        own_tile, own_res, side_tile, side_res = inputs
        own_part = jnp.dot(own_tile.T, own_res, preferred_element_type=jnp.float32)
        side_part = jnp.dot(side_tile.T, side_res, preferred_element_type=jnp.float32)
        return own_part + side_part

    near_part = lax.map(near_block, (self_tiles.reshape(cluster_groups, sample_points, sample_points), flattened_result, side_tiles.reshape(cluster_groups, sample_points, sample_points), neighbour.reshape(cluster_groups, sample_points, columns)))
    gradient = (near_part + distant_part).reshape(grid_rows, grid_cols, sample_points, columns)
    return gradient
```

```python
import jax
import jax.numpy as jnp
from jax import lax
from jax.experimental import pallas as pl
from jax.experimental.pallas import tpu as pltpu
from jax.sharding import PartitionSpec as P

MESH = pl.DeviceIdType.MESH
LEAF, K, NRHS, ADM = 2048, 32, 512, 64
CHUNKS = 16
ROWS = LEAF // CHUNKS
WINDOW = 3
BF, F32 = jnp.bfloat16, jnp.float32


def tdot(a, b):
    return lax.dot_general(a, b, (((0,), (0,)), ((), ())), preferred_element_type=F32)


def kernel(
    res, selft, sidet, rowb, colb, coup, side, targ, rank, count, out,
    res_v, self_v, side_v, rowb_v, colb_v, coup_v, side_s, targ_v, rank_v, count_v, nb_on, nb_off, nbs, acc,
    d32, dsend, m_v, g_v, pf, psend, r_v, fsend, f_v,
    lsem, osem, on_s, on_r, off_s, off_r, xp_s, xp_r, z_s, z_r, c_s, c_r, m_s, m_r, y_s, y_r, f_s, f_r,
):
    p, q = lax.axis_index("row"), lax.axis_index("col")
    c, x, z = p % 2, (p // 2) % 4, q // 2
    y = (p // 8) * 2 + q % 2
    xp, h = x % 2, x // 2

    def dev(x_, y_, z_, c_):
        return ((y_ // 2) * 8 + x_ * 2 + c_, z_ * 2 + y_ % 2)

    def load(k, src, dst):
        return pltpu.make_async_copy(src, dst, lsem.at[k])

    loads = [
        load(0, res, res_v), load(1, rowb, rowb_v), load(2, coup, coup_v),
        load(3, selft, self_v), load(4, sidet, side_v), load(5, colb, colb_v),
        load(6, side, side_s), load(7, targ, targ_v), load(8, rank, rank_v), load(9, count, count_v),
    ]
    for cp in loads:
        cp.start()

    group = []
    for k in range(1, 16):
        dc, dz, dx = k // 8, (k // 2) % 4, k % 2
        c2, x2 = (c + dc) % 2, (xp + dx) % 2
        z_to, z_from = (z + dz) % 4, (z + 4 - dz) % 4
        group.append((k, dev(2 * h + x2, y, z_to, c2), c2 * 8 + z_to * 2 + x2, c2 * 8 + z_from * 2 + x2))
    off_dev = ((p + 15 + 2 * c) % 16, q)
    on_dev = (p + 1 - 2 * c, q)
    y_devs = [dev(x, (y + k) % 4, z, c) for k in (1, 2, 3)]
    far_dev = dev(3 - x, y, z, c)
    bar = pltpu.get_barrier_semaphore()
    partners = [g[1] for g in group] + [off_dev, far_dev] + y_devs
    for d in partners:
        pl.semaphore_signal(bar, 1, device_id=d, device_id_type=MESH)

    me = c * 8 + z * 2 + xp
    loads[0].wait()
    loads[1].wait()
    g_v[me] = jnp.dot(rowb_v[...], res_v[...], preferred_element_type=F32).astype(BF)

    def rdma(src, dst, s, r, d):
        return pltpu.make_async_remote_copy(
            src_ref=src, dst_ref=dst, send_sem=s, recv_sem=r, device_id=d, device_id_type=MESH
        )

    def off(k):
        rows = pl.ds(k * ROWS, ROWS)
        return rdma(res_v.at[rows], nb_off.at[rows], off_s.at[k], off_r.at[k], off_dev)

    def pump(k):
        if k < CHUNKS:
            if k >= WINDOW:
                off(k - WINDOW).wait_send()
            off(k).start()

    on = rdma(res_v, nb_on, on_s, on_r, on_dev)
    xp_copy = rdma(g_v.at[me], g_v.at[me], xp_s, xp_r, dev(4 * h + 1 - x, y, z, c))

    pl.semaphore_wait(bar, len(partners))
    xp_copy.start()
    for k in range(WINDOW):
        pump(k)
    on.start()

    for cp in loads[6:]:
        cp.wait()
    loads[2].wait()
    rank_row = rank_v[0:1, :]
    r = lax.broadcasted_iota(jnp.int32, (128, ADM), 0)
    s_i = lax.broadcasted_iota(jnp.int32, (128, ADM), 1)
    t, d = r // 16, r % 16
    y2, nf = t // 2, t % 2
    c2, z2, x2 = d // 8, (d // 2) % 4, 2 * h + d % 2
    x3 = jnp.where(nf == 0, x2, 3 - x2)
    j = ((y2 // 2) * 8 + x3 * 2 + c2) * 8 + z2 * 2 + y2 % 2
    hit = jnp.where((targ_v[0:1, :] == j) & (s_i < count_v[0:1, 0:1]), rank_row, 0)
    mask_b = (r % K < rank_row).astype(F32)
    lane16 = lax.broadcasted_iota(jnp.int32, (16, 128), 1)

    def dense(a, _):
        lhs = jnp.where(hit > a, 1.0, 0.0).astype(BF)
        block = coup_v[pl.ds(pl.multiple_of(a * K, K), K), :].astype(F32)
        rhs = (jnp.concatenate([block] * 4, axis=0) * mask_b).astype(BF)
        full = lax.dot_general(lhs, rhs, (((1,), (1,)), ((), ())), preferred_element_type=F32)
        for u in range(2):
            got = jnp.zeros((16, 128), F32)
            for i in range(4):
                got = jnp.where(lane16 // K == i, full[(4 * u + i) * 16:(4 * u + i + 1) * 16, :], got)
            d32[u, pl.ds(a, 16, stride=K), :] = got
        return 0

    lax.fori_loop(0, K, dense, 0)
    for u in range(2):
        dsend[:, :, u * 128:(u + 1) * 128] = d32[u].reshape(16, K, 128).astype(BF)
    m_v[me] = dsend[me]
    m_copies = [rdma(dsend.at[to], m_v.at[me], m_s.at[k - 1], m_r.at[k - 1], d_) for k, d_, to, _ in group]
    for cp in m_copies:
        cp.start()
    pump(3)
    pump(4)

    xp_copy.wait_recv()
    mine = pl.ds(c * 8 + z * 2, 2)
    z_copies = [
        rdma(g_v.at[mine], g_v.at[mine], z_s.at[k - 1], z_r.at[k - 1], dev(x, y, (z + k) % 4, c)) for k in (1, 2, 3)
    ]
    for cp in z_copies:
        cp.start()
    pump(5)

    loads[3].wait()

    def self_part(i, _):
        cols = pl.ds(pl.multiple_of(i * 256, 256), 256)
        acc[cols, :] = tdot(self_v[:, cols], res_v[...])
        return 0

    lax.fori_loop(0, 4, self_part, 0)
    pump(6)
    for cp in z_copies:
        cp.wait_recv()
    half = pl.ds(c * 8, 8)
    c_copy = rdma(g_v.at[half], g_v.at[half], c_s, c_r, on_dev)
    c_copy.start()
    for cp in m_copies:
        cp.wait_recv()
    c_copy.wait_recv()
    pf[...] = tdot(m_v[...].reshape(512, 256), g_v[...].reshape(512, NRHS))
    psend[...] = pf[...].reshape(4, 2 * K, NRHS).astype(BF)
    y_copies = [
        rdma(psend.at[(y + k) % 4], r_v.at[y], y_s.at[k - 1], y_r.at[k - 1], y_devs[k - 1]) for k in (1, 2, 3)
    ]
    for cp in y_copies:
        cp.start()
    pump(7)
    lax.fori_loop(4, 8, self_part, 0)
    pump(8)

    near = side_s[0:1, 0:1]
    w_on = jnp.broadcast_to(jnp.where(near == 1 - 2 * c, 1.0, 0.0), (1, NRHS)).astype(BF)
    w_off = jnp.broadcast_to(jnp.where(near == 2 * c - 1, 1.0, 0.0), (1, NRHS)).astype(BF)
    on.wait_recv()
    loads[4].wait()

    def side_group(g):
        off(2 * g).wait_recv()
        off(2 * g + 1).wait_recv()
        rows = pl.ds(g * 256, 256)
        nbs[...] = nb_on[rows, :] * w_on + nb_off[rows, :] * w_off

    def side_tile(g, i):
        cols = pl.ds(pl.multiple_of(i * 512, 512), 512)
        acc[cols, :] += tdot(side_v[pl.ds(g * 256, 256), cols], nbs[...])

    def side_part(g):
        side_group(g)

        def body(i, _):
            side_tile(g, i)
            return 0

        lax.fori_loop(0, 4, body, 0)

    side_part(0)
    pump(9)
    side_part(1)
    pump(10)
    side_part(2)
    pump(11)
    pump(12)

    for cp in y_copies:
        cp.wait_recv()
    total = pf[pl.ds(pl.multiple_of(y * 2 * K, 2 * K), 2 * K), :]
    for k in (1, 2, 3):
        total = total + r_v[(y + k) % 4].astype(F32)
    pf[0:2 * K, :] = total
    fsend[...] = total[K:, :].astype(BF)
    far = rdma(fsend, f_v, f_s, f_r, far_dev)
    far.start()
    side_part(3)
    pump(13)
    pump(14)
    far.wait_recv()
    loads[5].wait()
    dual = (pf[0:K, :] + f_v[...].astype(F32)).astype(BF)

    def distant(i, _):
        rows = pl.ds(pl.multiple_of(i * 512, 512), 512)
        acc[rows, :] += tdot(colb_v[:, rows], dual)
        return 0

    lax.fori_loop(0, 4, distant, 0)
    side_part(4)
    pump(15)
    side_part(5)
    side_part(6)
    side_group(7)

    def put(i):
        rows = pl.ds(pl.multiple_of(i * 512, 512), 512)
        return pltpu.make_async_copy(acc.at[rows], out.at[rows], osem.at[i])

    def last(i, _):
        side_tile(7, i)
        put(i).start()
        return 0

    lax.fori_loop(0, 4, last, 0)
    for k in range(CHUNKS - WINDOW, CHUNKS):
        off(k).wait_send()
    for cp in [on, xp_copy, c_copy, far] + z_copies + m_copies + y_copies:
        cp.wait_send()
    for i in range(4):
        put(i).wait()


def on_device(*args):
    res, selft, sidet, rowb, colb, coup, side, targ, rank, count = args
    anyspace = pl.BlockSpec(memory_space=pl.ANY)
    dma = pltpu.SemaphoreType.DMA
    out = pl.pallas_call(
        kernel,
        out_shape=jax.ShapeDtypeStruct((LEAF, NRHS), F32),
        in_specs=[anyspace] * 10,
        out_specs=anyspace,
        scratch_shapes=[
            pltpu.VMEM((LEAF, NRHS), BF),
            pltpu.VMEM((LEAF, LEAF), BF),
            pltpu.VMEM((LEAF, LEAF), BF),
            pltpu.VMEM((K, LEAF), BF),
            pltpu.VMEM((K, LEAF), BF),
            pltpu.VMEM((K * K, ADM), BF),
            pltpu.VMEM((1, 1), jnp.int32),
            pltpu.VMEM((1, ADM), jnp.int32),
            pltpu.VMEM((1, ADM), jnp.int32),
            pltpu.VMEM((1, 1), jnp.int32),
            pltpu.VMEM((LEAF, NRHS), BF),
            pltpu.VMEM((LEAF, NRHS), BF),
            pltpu.VMEM((256, NRHS), BF),
            pltpu.VMEM((LEAF, NRHS), F32),
            pltpu.VMEM((2, 16 * K, 128), F32),
            pltpu.VMEM((16, K, 256), BF),
            pltpu.VMEM((16, K, 256), BF),
            pltpu.VMEM((16, K, NRHS), BF),
            pltpu.VMEM((256, NRHS), F32),
            pltpu.VMEM((4, 2 * K, NRHS), BF),
            pltpu.VMEM((4, 2 * K, NRHS), BF),
            pltpu.VMEM((K, NRHS), BF),
            pltpu.VMEM((K, NRHS), BF),
            dma((10,)), dma((4,)), dma, dma, dma((CHUNKS,)), dma((CHUNKS,)), dma, dma,
            dma((3,)), dma((3,)), dma, dma, dma((15,)), dma((15,)), dma((3,)), dma((3,)), dma, dma,
        ],
        compiler_params=pltpu.CompilerParams(
            collective_id=0, has_side_effects=True, vmem_limit_bytes=63 * 2**20
        ),
    )(
        res[0, 0], selft[0, 0], sidet[0, 0], rowb[0, 0].T, colb[0, 0].T,
        coup[0, 0].transpose(1, 2, 0).reshape(K * K, ADM),
        side, targ[0], rank[0], count,
    )
    return out[None, None]


def solution(mesh):
    rc = ("row", "col")
    in_specs = tuple(P(*rc, *[None] * n) for n in (2, 2, 2, 2, 2, 3, 0, 1, 1, 0))
    return jax.shard_map(
        on_device, mesh=mesh, in_specs=in_specs, out_specs=P(*rc, None, None), check_vma=False
    )
```

```python
import jax
import jax.numpy as jnp
from jax import lax
from jax.experimental import pallas as pl
from jax.experimental.pallas import tpu as pltpu
from jax.sharding import PartitionSpec as P

MESH = pl.DeviceIdType.MESH
LEAF, K, NRHS, ADM = 2048, 32, 512, 64
HALF = NRHS // 2
BF, F32 = jnp.bfloat16, jnp.float32
PIECES = [(0, i * 512, 512) for i in range(4)] + [(1, i * 512, 512) for i in range(3)] + [(1, 1536, 256), (1, 1792, 256)]
LAST = 256


def tdot(a, b):
    return lax.dot_general(a, b, (((0,), (0,)), ((), ())), preferred_element_type=F32)


def scope(name):
    return jax.named_scope(name)


def kernel(
    res, selft, sidet, rowb, colb, coup, targ, rank, side, count,
    acc, side_v, nbl, colb_v, dual,
    res_v, self_v, rowb_v, coup_v, targ_v, rank_v, side_s, count_v, nb_on, nb_off,
    targ_r, raw_s, raw_r, d32, dsend, m_v, g_v, pf, psend, r_v, qs, f_v, n_v,
    lsem, on_s, on_r, off_s, off_r, xp_s, xp_r, z_s, z_r, c_s, c_r, m_s, m_r, y_s, y_r, f_s, f_r, n_s, n_r, w_s, w_r,
):
    p, q = lax.axis_index("row"), lax.axis_index("col")
    c, x, z = p % 2, (p // 2) % 4, q // 2
    y = (p // 8) * 2 + q % 2
    xp, h = x % 2, x // 2
    hx = 1 + h
    handler = x == hx
    near_core = hx % 2

    def dev(x_, y_, z_, c_):
        return ((y_ // 2) * 8 + x_ * 2 + c_, z_ * 2 + y_ % 2)

    off_dev = ((p + 15 + 2 * c) % 16, q)
    on_dev = (p + 1 - 2 * c, q)
    y_devs = [dev(x, (y + k) % 4, z, c) for k in (1, 2, 3)]
    side_x = 4 * h + 1 - x
    far_devs = [dev(2 - 2 * h + k // 2, y, z, k % 2) for k in range(4)]
    outer_dev = dev(hx, y, z, c)
    bar = pltpu.get_barrier_semaphore()
    common = [off_dev, dev(side_x, y, z, 0), dev(side_x, y, z, 1)]
    peers = [dev(x, y, (z + k % 4) % 4, (c + k // 4) % 2) for k in range(1, 8)]
    inner = common + far_devs + y_devs + peers
    outer = common + [on_dev] + [dev(2 - h, y, z, 0), dev(2 - h, y, z, 1)]

    @pl.when(handler)
    def _():
        for d in inner:
            pl.semaphore_signal(bar, 1, device_id=d, device_id_type=MESH)

    @pl.when(jnp.logical_not(handler))
    def _():
        for d in outer:
            pl.semaphore_signal(bar, 1, device_id=d, device_id_type=MESH)

    def load(k, src, dst):
        return pltpu.make_async_copy(src, dst, lsem.at[k])

    loads = [
        load(0, res.at[:, :HALF], res_v.at[0]), load(1, res.at[:, HALF:], res_v.at[1]), load(2, rowb, rowb_v),
        load(3, coup, coup_v), load(4, targ, targ_v), load(5, rank, rank_v), load(6, count, count_v),
        load(7, selft, self_v), load(8, sidet, side_v), load(9, colb, colb_v), load(10, side, side_s),
    ]
    for k in (3, 4, 5, 6, 2, 0, 1, 10, 7, 8, 9):
        loads[k].start()

    with scope("A_wload"):
        for cp in loads[3:7]:
            cp.wait()
    r = lax.broadcasted_iota(jnp.int32, (K * K, ADM), 0)
    s_i = lax.broadcasted_iota(jnp.int32, (K * K, ADM), 1)
    live = (jnp.maximum(r // K, r % K) < rank_v[0:1, :]) & (s_i < count_v[0:1, 0:1])
    masked = jnp.where(live, coup_v[...].astype(F32), 0.0)
    raw_s[...] = jnp.concatenate([masked[:512], masked[512:]], axis=1).astype(BF)

    lane = lax.broadcasted_iota(jnp.int32, (8, 128), 1)

    def densify(raw, targets, slot):
        r = lax.broadcasted_iota(jnp.int32, (256, 128), 0)
        at = lax.broadcasted_iota(jnp.int32, (256, 128), 1) // ADM == r // 128
        t, d = (r // 8) % 16, r % 8
        c2, z2 = d // 4, d % 4
        x3 = jnp.where(c2 == near_core, 2 * h, 2 - 2 * h) + (t // 2) % 2
        y2, ct = t // 4, t % 2
        j = ((y2 // 2) * 8 + x3 * 2 + ct) * 8 + z2 * 2 + y2 % 2
        row = targets[0:1, :]
        hit = jnp.where((jnp.concatenate([row, row], axis=1) == j) & at, 1.0, 0.0).astype(BF)

        def body(a, _):
            block = raw[pl.ds(pl.multiple_of(a * K, K), K), :]
            full = lax.dot_general(
                hit, jnp.concatenate([block] * 4, axis=0), (((1,), (1,)), ((), ())), preferred_element_type=F32
            )
            for v in range(2):
                for u in range(4):
                    got = jnp.zeros((8, 128), F32)
                    for i in range(4):
                        at = (16 * v + 4 * u + i) * 8
                        got = jnp.where(lane // K == i, full[at:at + 8, :], got)
                    d32[u, pl.ds(a + 16 * v, 8, stride=K), :] = got
            return 0

        lax.fori_loop(0, 16, body, 0, unroll=4)
        for u in range(4):
            dsend[slot, :, :, u * 128:(u + 1) * 128] = d32[u].reshape(8, K, 128).astype(BF)

    @pl.when(handler)
    def _():
        with scope("B_dense"):
            densify(raw_s, targ_v, 0)

    me = c * 8 + z * 2 + xp
    mate = c * 8 + z * 2 + 1 - xp

    with scope("C_coef"):
        for k in (2, 0, 1):
            loads[k].wait()
        for u in range(2):
            g_v[me, :, u * HALF:(u + 1) * HALF] = jnp.dot(
                rowb_v[...], res_v[u], preferred_element_type=F32
            ).astype(BF)

    def rdma(src, dst, s, r, d):
        return pltpu.make_async_remote_copy(
            src_ref=src, dst_ref=dst, send_sem=s, recv_sem=r, device_id=d, device_id_type=MESH
        )

    def off(k):
        u, r0, n = PIECES[k]
        rows = pl.ds(r0, n)
        return rdma(res_v.at[u, rows], nb_off.at[u, rows], off_s.at[k], off_r.at[k], off_dev)

    offs = [off(k) for k in range(len(PIECES))]
    on = rdma(res_v, nb_on, on_s, on_r, on_dev)
    xp_copy = rdma(g_v.at[me], g_v.at[me], xp_s, xp_r, outer_dev)
    raw_copy = rdma(raw_s, raw_r, w_s.at[0], w_r.at[0], outer_dev)
    targ_copy = rdma(targ_v, targ_r, w_s.at[1], w_r.at[1], outer_dev)
    m_copies = []
    for i, src in enumerate((me, mate)):
        for k in range(1, 8):
            c2, z2 = (c + k // 4) % 2, (z + k) % 4
            m_copies.append(
                rdma(dsend.at[i, c2 * 4 + z2], m_v.at[src], m_s.at[i, k], m_r.at[i, k], dev(hx, y, z2, c2))
            )

    with scope("D_bar"):
        @pl.when(handler)
        def _():
            pl.semaphore_wait(bar, len(inner))

        @pl.when(jnp.logical_not(handler))
        def _():
            pl.semaphore_wait(bar, len(outer))


    @pl.when(handler)
    def _():
        for cp in m_copies[:7]:
            cp.start()
        m_v[me] = dsend[0, c * 4 + z]

    @pl.when(jnp.logical_not(handler))
    def _():
        for cp in (xp_copy, targ_copy, raw_copy):
            cp.start()

    for cp in offs:
        cp.start()
    on.start()

    def self_part(i, _):
        cols = pl.ds(pl.multiple_of(i * 256, 256), 256)
        got = tdot(self_v[:, cols], jnp.concatenate([res_v[0], res_v[1]], axis=1))
        acc[0, cols, :] = got[:, :HALF]
        acc[1, cols, :] = got[:, HALF:]
        return 0

    with scope("E_wself"):
        loads[7].wait()
    mine = pl.ds(c * 8 + z * 2, 2)
    z_copies = [
        rdma(g_v.at[mine], g_v.at[mine], z_s.at[k - 1], z_r.at[k - 1], dev(x, y, (z + k) % 4, c)) for k in (1, 2, 3)
    ]
    half = pl.ds(c * 8, 8)
    c_copy = rdma(g_v.at[half], g_v.at[half], c_s, c_r, on_dev)
    y_copies = [
        rdma(psend.at[(y + k) % 4], r_v.at[y], y_s.at[k - 1], y_r.at[k - 1], y_devs[k - 1]) for k in (1, 2, 3)
    ]
    near_is_me = c == near_core
    far = [rdma(qs.at[k], f_v, f_s.at[k], f_r, far_devs[k]) for k in range(4)]
    near = [rdma(qs.at[xp * 2 + 1 - c], n_v, n_s.at[0], n_r, on_dev)] + [
        rdma(qs.at[(1 - xp) * 2 + k], n_v, n_s.at[1 + k], n_r, dev(side_x, y, z, k)) for k in (0, 1)
    ]

    with scope("E_self1"):
        lax.fori_loop(0, 3, self_part, 0, unroll=3)

    @pl.when(handler)
    def _():
        with scope("F_wxp"):
            xp_copy.wait_recv()
        for cp in z_copies:
            cp.start()
        with scope("F_wraw"):
            targ_copy.wait_recv()
            raw_copy.wait_recv()
        with scope("F_dense"):
            densify(raw_r, targ_r, 1)
        for cp in m_copies[7:]:
            cp.start()
        m_v[mate] = dsend[1, c * 4 + z]

    with scope("F_self2"):
        lax.fori_loop(3, 6, self_part, 0, unroll=3)

    @pl.when(handler)
    def _():
        with scope("H_wz"):
            for cp in z_copies:
                cp.wait_recv()
        c_copy.start()

    with scope("H_self3"):
        lax.fori_loop(6, 8, self_part, 0, unroll=2)

    @pl.when(handler)
    def _():
        with scope("I_wm"):
            for cp in m_copies:
                cp.wait_recv()
        with scope("I_wc"):
            c_copy.wait_recv()
        with scope("I_pf"):
            pf[...] = tdot(m_v[...].reshape(512, 512), g_v[...].reshape(512, NRHS))
            psend[...] = pf[...].reshape(4, 4 * K, NRHS).astype(BF)
        for cp in y_copies:
            cp.start()

    loads[10].wait()
    which = side_s[0:1, 0:1]
    w_on = jnp.broadcast_to(jnp.where(which == 1 - 2 * c, 1.0, 0.0), (1, HALF)).astype(BF)
    w_off = jnp.broadcast_to(jnp.where(which == 2 * c - 1, 1.0, 0.0), (1, HALF)).astype(BF)
    with scope("G_won"):
        on.wait_recv()
        loads[8].wait()

    def picked(k):
        u, r0, n = PIECES[k]
        rows = pl.ds(r0, n)
        with scope(f"w{k}"):
            offs[k].wait_recv()
        return nb_on[u, rows, :] * w_on + nb_off[u, rows, :] * w_off

    def side_part(k):
        u, r0, n = PIECES[k]
        nbl[pl.ds(0, n), :] = picked(k)
        with scope(f"S{k}"):
            def body(i, _):
                cols = pl.ds(pl.multiple_of(i * 512, 512), 512)
                acc[u, cols, :] += tdot(side_v[pl.ds(r0, n), cols], nbl[pl.ds(0, n), :])
                return 0

            lax.fori_loop(0, 4, body, 0, unroll=4)

    side_part(0)
    side_part(1)
    side_part(2)
    side_part(3)

    @pl.when(handler)
    def _():
        with scope("K_wy"):
            for cp in y_copies:
                cp.wait_recv()
        total = pf[pl.ds(pl.multiple_of(y * 4 * K, 4 * K), 4 * K), :]
        for k in (1, 2, 3):
            total = total + r_v[(y + k) % 4].astype(F32)
        qs[...] = total.astype(BF).reshape(4, K, NRHS)

        @pl.when(near_is_me)
        def _():
            for cp in near:
                cp.start()
            n_v[...] = qs[xp * 2 + c]

        @pl.when(jnp.logical_not(near_is_me))
        def _():
            for cp in far:
                cp.start()

    side_part(4)
    side_part(5)
    side_part(6)
    side_part(7)
    with scope("Q_sends"):
        for cp in offs + [on]:
            cp.wait_send()

        @pl.when(handler)
        def _():
            for cp in m_copies + z_copies + [c_copy] + y_copies:
                cp.wait_send()

            @pl.when(near_is_me)
            def _():
                for cp in near:
                    cp.wait_send()

            @pl.when(jnp.logical_not(near_is_me))
            def _():
                for cp in far:
                    cp.wait_send()

        @pl.when(jnp.logical_not(handler))
        def _():
            for cp in (xp_copy, targ_copy, raw_copy):
                cp.wait_send()

    nbl[pl.ds(0, LAST), :] = picked(8)
    with scope("M_wdual"):
        far[0].wait_recv()

        @pl.when(jnp.logical_not(handler & near_is_me))
        def _():
            near[0].wait_recv()

    loads[9].wait()
    dual[...] = (n_v[...].astype(F32) + f_v[...].astype(F32)).astype(BF)


def finish(acc, side_v, nbl, colb_v, dual, out, tmp, sem):
    copies = []
    for u in range(2):
        for i in range(4):
            rows = pl.ds(i * 512, 512)
            got = acc[u, rows, :] + tdot(colb_v[:, rows], dual[:, u * HALF:(u + 1) * HALF])
            if u:
                got = got + tdot(side_v[pl.ds(LEAF - LAST, LAST), rows], nbl[pl.ds(0, LAST), :])
            tmp[u, rows, :] = got
            cp = pltpu.make_async_copy(tmp.at[u, rows], out.at[rows, pl.ds(u * HALF, HALF)], sem.at[u * 4 + i])
            cp.start()
            copies.append(cp)
    for cp in copies:
        cp.wait()


def on_device(*args):
    res, selft, sidet, rowb, colb, coup, side, targ, rank, count = args
    anyspace = pl.BlockSpec(memory_space=pl.ANY)
    vm = pl.BlockSpec(memory_space=pltpu.VMEM)
    hbm = pl.BlockSpec(memory_space=pltpu.HBM)
    dma = pltpu.SemaphoreType.DMA
    n = len(PIECES)
    ins = (
        res[0, 0], selft[0, 0], sidet[0, 0], rowb[0, 0].T, colb[0, 0].T,
        coup[0, 0].transpose(1, 2, 0).reshape(K * K, ADM), targ[0], rank[0], side, count,
    )
    ins = [a if a.size == 1 else pltpu.with_memory_space_constraint(a, pltpu.HBM) for a in ins]
    mid = pl.pallas_call(
        kernel,
        out_shape=[
            pltpu.VMEM((2, LEAF, HALF), F32), pltpu.VMEM((LEAF, LEAF), BF), pltpu.VMEM((512, HALF), BF),
            pltpu.VMEM((K, LEAF), BF), pltpu.VMEM((K, NRHS), BF),
        ],
        in_specs=[hbm] * 8 + [anyspace] * 2,
        out_specs=[vm] * 5,
        scratch_shapes=[
            pltpu.VMEM((2, LEAF, HALF), BF),
            pltpu.VMEM((LEAF, LEAF), BF),
            pltpu.VMEM((K, LEAF), BF),
            pltpu.VMEM((K * K, ADM), BF),
            pltpu.VMEM((1, ADM), jnp.int32),
            pltpu.VMEM((1, ADM), jnp.int32),
            pltpu.VMEM((1, 1), jnp.int32),
            pltpu.VMEM((1, 1), jnp.int32),
            pltpu.VMEM((2, LEAF, HALF), BF),
            pltpu.VMEM((2, LEAF, HALF), BF),
            pltpu.VMEM((1, ADM), jnp.int32),
            pltpu.VMEM((512, 128), BF),
            pltpu.VMEM((512, 128), BF),
            pltpu.VMEM((4, 8 * K, 128), F32),
            pltpu.VMEM((2, 8, K, 512), BF),
            pltpu.VMEM((16, K, 512), BF),
            pltpu.VMEM((16, K, NRHS), BF),
            pltpu.VMEM((512, NRHS), F32),
            pltpu.VMEM((4, 4 * K, NRHS), BF),
            pltpu.VMEM((4, 4 * K, NRHS), BF),
            pltpu.VMEM((4, K, NRHS), BF),
            pltpu.VMEM((K, NRHS), BF),
            pltpu.VMEM((K, NRHS), BF),
            dma((11,)), dma, dma, dma((n,)), dma((n,)), dma, dma, dma((3,)), dma((3,)), dma, dma,
            dma((2, 8)), dma((2, 8)), dma((3,)), dma((3,)), dma((4,)), dma, dma((3,)), dma, dma((2,)), dma((2,)),
        ],
        compiler_params=pltpu.CompilerParams(
            collective_id=0, has_side_effects=True, vmem_limit_bytes=36 * 2**20
        ),
    )(*ins)
    out = pl.pallas_call(
        finish,
        out_shape=jax.ShapeDtypeStruct((LEAF, NRHS), F32),
        in_specs=[vm] * 5,
        out_specs=anyspace,
        scratch_shapes=[pltpu.VMEM((2, LEAF, HALF), F32), dma((8,))],
        compiler_params=pltpu.CompilerParams(vmem_limit_bytes=12 * 2**20),
    )(*mid)
    return out[None, None]


def solution(mesh):
    rc = ("row", "col")
    in_specs = tuple(P(*rc, *[None] * n) for n in (2, 2, 2, 2, 2, 3, 0, 1, 1, 0))
    return jax.shard_map(
        on_device, mesh=mesh, in_specs=in_specs, out_specs=P(*rc, None, None), check_vma=False
    )
```

```python
import jax
import jax.numpy as jnp
from jax import lax
from jax.experimental import pallas as pl
from jax.experimental.pallas import tpu as pltpu
from jax.sharding import PartitionSpec as P

MESH = pl.DeviceIdType.MESH
LEAF, K, NRHS, ADM = 2048, 32, 512, 64
HALF = NRHS // 2
BF, F32 = jnp.bfloat16, jnp.float32
PIECES = [(0, i * 512, 512) for i in range(4)] + [(1, i * 512, 512) for i in range(3)] + [(1, 1536, 256), (1, 1792, 256)]
LAST = 256


def tdot(a, b):
    return lax.dot_general(a, b, (((0,), (0,)), ((), ())), preferred_element_type=F32)


def scope(name):
    return jax.named_scope(name)


def kernel(
    res, selft, sidet, rowb, colb, coup, targ, rank, side, count,
    acc, side_v, nbl, colb_v, dual,
    res_v, self_v, rowb_v, coup_v, targ_v, rank_v, side_s, count_v, nb_on, nb_off,
    targ_r, raw_s, raw_r, d32, ds_a, ds_b, m_a, m_b, g_v, p32, p2, ps, q_v, r_v, qs, f_v, n_v,
    lsem, ssem, off_r, on_r, xp_r, w_r, z_r, c_r, m_r, q_r, y_r, f_r, n_r,
):
    p, q = lax.axis_index("row"), lax.axis_index("col")
    c, x, z = p % 2, (p // 2) % 4, q // 2
    y = (p // 8) * 2 + q % 2
    xp, h = x % 2, x // 2
    hx = 1 + h
    handler = x == hx
    near_core = hx % 2

    def dev(x_, y_, z_, c_):
        return ((y_ // 2) * 8 + x_ * 2 + c_, z_ * 2 + y_ % 2)

    off_dev = ((p + 15 + 2 * c) % 16, q)
    on_dev = (p + 1 - 2 * c, q)
    y_devs = [dev(x, (y + k) % 4, z, c) for k in (1, 2, 3)]
    side_x = 4 * h + 1 - x
    far_devs = [dev(2 - 2 * h + k // 2, y, z, k % 2) for k in range(4)]
    outer_dev = dev(hx, y, z, c)
    bar = pltpu.get_barrier_semaphore()
    common = [off_dev, dev(side_x, y, z, 0), dev(side_x, y, z, 1)]
    peers = [dev(x, y, (z + k % 4) % 4, (c + k // 4) % 2) for k in range(1, 8)]
    inner = common + far_devs + y_devs + peers
    outer = common + [on_dev] + [dev(2 - h, y, z, 0), dev(2 - h, y, z, 1)]

    @pl.when(handler)
    def _():
        for d in inner:
            pl.semaphore_signal(bar, 1, device_id=d, device_id_type=MESH)

    @pl.when(jnp.logical_not(handler))
    def _():
        for d in outer:
            pl.semaphore_signal(bar, 1, device_id=d, device_id_type=MESH)

    def load(k, src, dst):
        return pltpu.make_async_copy(src, dst, lsem.at[k])

    def done(ref, sem):
        pltpu.make_async_copy(ref, ref, sem).wait()

    small = [load(0, coup, coup_v), load(1, targ, targ_v), load(2, rank, rank_v), load(3, count, count_v), load(4, side, side_s)]
    load_rowb = load(5, rowb, rowb_v)
    first = [load_rowb, load(6, res.at[:, :HALF], res_v.at[0]), load(6, res.at[:, HALF:], res_v.at[1])]
    load_self, load_side, load_colb = load(7, selft, self_v), load(8, sidet, side_v), load(9, colb, colb_v)
    for cp in first + small + [load_self]:
        cp.start()

    with scope("A_wload"):
        for cp in small:
            cp.wait()
    r = lax.broadcasted_iota(jnp.int32, (K * K, ADM), 0)
    s_i = lax.broadcasted_iota(jnp.int32, (K * K, ADM), 1)
    live = (jnp.maximum(r // K, r % K) < rank_v[0:1, :]) & (s_i < count_v[0:1, 0:1])
    masked = jnp.where(live, coup_v[...].astype(F32), 0.0)
    raw_s[...] = jnp.concatenate([masked[:512], masked[512:]], axis=1).astype(BF)

    lane = lax.broadcasted_iota(jnp.int32, (8, 128), 1)

    def densify(raw, targets, slot, ready=None):
        r = lax.broadcasted_iota(jnp.int32, (256, 128), 0)
        at = lax.broadcasted_iota(jnp.int32, (256, 128), 1) // ADM == r // 128
        t, d = (r // 8) % 16, r % 8
        c2, z2 = d // 4, d % 4
        x3 = jnp.where(c2 == near_core, 2 * h, 2 - 2 * h) + (t // 2) % 2
        kk, ct = t // 4, t % 2
        y2 = (y + jnp.where(kk == 0, 2, jnp.where(kk == 1, 1, jnp.where(kk == 2, 3, 0)))) % 4
        j = ((y2 // 2) * 8 + x3 * 2 + ct) * 8 + z2 * 2 + y2 % 2
        row = targets[0:1, :]
        hit = jnp.where((jnp.concatenate([row, row], axis=1) == j) & at, 1.0, 0.0).astype(BF)

        def body(a, _):
            block = raw[pl.ds(pl.multiple_of(a * K, K), K), :]
            full = lax.dot_general(
                hit, jnp.concatenate([block] * 4, axis=0), (((1,), (1,)), ((), ())), preferred_element_type=F32
            )
            for v in range(2):
                for u in range(4):
                    got = jnp.zeros((8, 128), F32)
                    for i in range(4):
                        at = (16 * v + 4 * u + i) * 8
                        got = jnp.where(lane // K == i, full[at:at + 8, :], got)
                    d32[u, pl.ds(a + 16 * v, 8, stride=K), :] = got
            return 0

        lax.fori_loop(0, 8, body, 0, unroll=4)
        if ready is not None:
            ready()
        lax.fori_loop(8, 16, body, 0, unroll=4)
        ds_a[slot] = d32[0].reshape(8, K, 128).astype(BF)
        for u in range(3):
            ds_b[slot, :, :, u * 128:(u + 1) * 128] = d32[1 + u].reshape(8, K, 128).astype(BF)

    mine, mate = c * 8 + z, c * 8 + 4 + z
    me = jnp.where(handler, mine, mate)

    with scope("C_coef"):
        load_rowb.wait()
        done(res_v, lsem.at[6])
        for u in range(2):
            g_v[me, :, u * HALF:(u + 1) * HALF] = jnp.dot(
                rowb_v[...], res_v[u], preferred_element_type=F32
            ).astype(BF)

    def rdma(src, dst, s, r, d):
        return pltpu.make_async_remote_copy(
            src_ref=src, dst_ref=dst, send_sem=s, recv_sem=r, device_id=d, device_id_type=MESH
        )

    def off(k):
        u, r0, n = PIECES[k]
        rows = pl.ds(r0, n)
        return rdma(res_v.at[u, rows], nb_off.at[u, rows], ssem.at[0], off_r.at[k], off_dev)

    offs = [off(k) for k in range(len(PIECES))]
    on = rdma(res_v, nb_on, ssem.at[7], on_r, on_dev)
    xp_copy = rdma(g_v.at[me], g_v.at[me], ssem.at[8], xp_r, outer_dev)
    raw_copies = [
        rdma(raw_s.at[pl.ds(i * 256, 256)], raw_r.at[pl.ds(i * 256, 256)], ssem.at[1], w_r.at[i], outer_dev) for i in (0, 1)
    ]
    targ_copy = rdma(targ_v, targ_r, ssem.at[9], w_r.at[2], outer_dev)
    m_copies = []
    for i, src in enumerate((mine, mate)):
        for l, (ds, m) in enumerate(((ds_a, m_a), (ds_b, m_b))):
            m_copies.append([
                rdma(
                    ds.at[i, (c + k // 4) % 2 * 4 + (z + k) % 4], m.at[src], ssem.at[2], m_r.at[l],
                    dev(hx, y, (z + k) % 4, (c + k // 4) % 2),
                ) for k in range(1, 8)
            ])
    z_copies = [
        [
            rdma(g_v.at[src], g_v.at[src], ssem.at[3], z_r.at[i], dev(x, y, (z + k) % 4, c))
            for k in (2, 1, 3)
        ] for i, src in enumerate((mine, mate))
    ]
    c_copies = []
    for i in range(2):
        part = pl.ds(c * 8 + 4 * i, 4)
        c_copies.append(rdma(g_v.at[part], g_v.at[part], ssem.at[4], c_r.at[i], on_dev))

    with scope("D_bar"):
        @pl.when(handler)
        def _():
            pl.semaphore_wait(bar, len(inner))

        @pl.when(jnp.logical_not(handler))
        def _():
            pl.semaphore_wait(bar, len(outer))


    @pl.when(handler)
    def _():
        for cp in z_copies[0]:
            cp.start()

    @pl.when(jnp.logical_not(handler))
    def _():
        for cp in [targ_copy] + raw_copies + [xp_copy]:
            cp.start()

    for cp in offs:
        cp.start()
    on.start()
    load_side.start()
    load_colb.start()

    @pl.when(handler)
    def _():
        with scope("B_dense"):
            densify(raw_s, targ_v, 0)
        for cp in m_copies[0] + m_copies[1]:
            cp.start()
        m_a[mine] = ds_a[0, c * 4 + z]
        m_b[mine] = ds_b[0, c * 4 + z]

    def self_part(i, _):
        cols = pl.ds(pl.multiple_of(i * 256, 256), 256)
        got = tdot(self_v[:, cols], jnp.concatenate([res_v[0], res_v[1]], axis=1))
        acc[0, cols, :] = got[:, :HALF]
        acc[1, cols, :] = got[:, HALF:]
        return 0

    with scope("E_wself"):
        load_self.wait()
    q_copies = [rdma(p2.at[k], q_v.at[k], ssem.at[5], q_r, y_devs[2 * k]) for k in (0, 1)]
    y_copies = [rdma(ps.at[k], r_v.at[k], ssem.at[5], y_r, y_devs[2 * k]) for k in (0, 1)]
    near_is_me = c == near_core
    far = [rdma(qs.at[k], f_v, ssem.at[6], f_r, far_devs[k]) for k in range(4)]
    near = [rdma(qs.at[xp * 2 + 1 - c], n_v, ssem.at[6], n_r, on_dev)] + [
        rdma(qs.at[(1 - xp) * 2 + k], n_v, ssem.at[6], n_r, dev(side_x, y, z, k)) for k in (0, 1)
    ]

    with scope("E_self1"):
        lax.fori_loop(0, 3, self_part, 0, unroll=3)

    @pl.when(handler)
    def _():
        with scope("F_wraw"):
            targ_copy.wait_recv()
            raw_copies[0].wait_recv()
        with scope("F_dense"):
            densify(raw_r, targ_r, 1, raw_copies[1].wait_recv)
        for cp in m_copies[2]:
            cp.start()
        with scope("F_wxp"):
            xp_copy.wait_recv()
        for cp in z_copies[1] + m_copies[3]:
            cp.start()
        m_a[mate] = ds_a[1, c * 4 + z]
        m_b[mate] = ds_b[1, c * 4 + z]
        with scope("F_wz"):
            done(g_v.at[pl.ds(0, 3)], z_r.at[0])
        c_copies[0].start()

    with scope("F_self2"):
        lax.fori_loop(3, 8, self_part, 0, unroll=5)

    @pl.when(handler)
    def _():
        with scope("H_wz"):
            done(g_v.at[pl.ds(0, 3)], z_r.at[1])
        c_copies[1].start()
        with scope("I_wma"):
            done(m_a.at[pl.ds(0, 14)], m_r.at[0])
        with scope("I_wc"):
            for cp in c_copies:
                cp.wait_recv()
        with scope("I_pa"):
            got = tdot(m_a[...].reshape(512, 128), g_v[...].reshape(512, NRHS)).astype(BF)
            p2[0] = got[:, :HALF]
            p2[1] = got[:, HALF:]
        for cp in q_copies:
            cp.start()
        with scope("I_wmb"):
            done(m_b.at[pl.ds(0, 14)], m_r.at[1])
        with scope("I_pb"):
            p32[...] = tdot(m_b[...].reshape(512, 384), g_v[...].reshape(512, NRHS)).reshape(3, 128, NRHS)

    which = side_s[0:1, 0:1]
    w_on = jnp.broadcast_to(jnp.where(which == 1 - 2 * c, 1.0, 0.0), (1, HALF)).astype(BF)
    w_off = jnp.broadcast_to(jnp.where(which == 2 * c - 1, 1.0, 0.0), (1, HALF)).astype(BF)
    with scope("G_won"):
        on.wait_recv()
        load_side.wait()

    def picked(k):
        u, r0, n = PIECES[k]
        rows = pl.ds(r0, n)
        with scope(f"w{k}"):
            offs[k].wait_recv()
        return nb_on[u, rows, :] * w_on + nb_off[u, rows, :] * w_off

    def side_part(k):
        u, r0, n = PIECES[k]
        nbl[pl.ds(0, n), :] = picked(k)
        with scope(f"S{k}"):
            def body(i, _):
                cols = pl.ds(pl.multiple_of(i * 512, 512), 512)
                acc[u, cols, :] += tdot(side_v[pl.ds(r0, n), cols], nbl[pl.ds(0, n), :])
                return 0

            lax.fori_loop(0, 4, body, 0, unroll=4)

    side_part(0)
    side_part(1)

    @pl.when(handler)
    def _():
        with scope("J_wq"):
            done(q_v, q_r)
        for k in range(2):
            cols = slice(k * HALF, (k + 1) * HALF)
            rest = slice((1 - k) * HALF, (2 - k) * HALF)
            ps[k, :, cols] = (p32[k, :, cols] + q_v[k].astype(F32)).astype(BF)
            ps[k, :, rest] = p32[k, :, rest].astype(BF)
            y_copies[k].start()

    side_part(2)
    side_part(3)

    @pl.when(handler)
    def _():
        with scope("K_wy"):
            done(r_v, y_r)
        total = p32[2] + r_v[0].astype(F32) + r_v[1].astype(F32)
        qs[...] = total.astype(BF).reshape(4, K, NRHS)

        @pl.when(near_is_me)
        def _():
            for cp in near:
                cp.start()
            n_v[...] = qs[xp * 2 + c]

        @pl.when(jnp.logical_not(near_is_me))
        def _():
            for cp in far:
                cp.start()

    side_part(4)
    side_part(5)
    side_part(6)
    side_part(7)
    with scope("Q_sends"):
        done(res_v, ssem.at[0])
        on.wait_send()

        @pl.when(handler)
        def _():
            done(g_v.at[pl.ds(0, 14)], ssem.at[2])
            done(g_v.at[pl.ds(0, 6)], ssem.at[3])
            done(g_v.at[pl.ds(0, 8)], ssem.at[4])
            done(g_v.at[pl.ds(0, 12)], ssem.at[5])

            @pl.when(near_is_me)
            def _():
                done(g_v.at[pl.ds(0, 3)], ssem.at[6])

            @pl.when(jnp.logical_not(near_is_me))
            def _():
                done(g_v.at[pl.ds(0, 4)], ssem.at[6])

        @pl.when(jnp.logical_not(handler))
        def _():
            done(raw_s, ssem.at[1])
            xp_copy.wait_send()
            targ_copy.wait_send()

    nbl[pl.ds(0, LAST), :] = picked(8)
    with scope("M_wfar"):
        far[0].wait_recv()

    with scope("M_wdual"):
        @pl.when(jnp.logical_not(handler & near_is_me))
        def _():
            near[0].wait_recv()

    load_colb.wait()
    dual[...] = (n_v[...].astype(F32) + f_v[...].astype(F32)).astype(BF)


def finish(acc, side_v, nbl, colb_v, dual, out, tmp, sem):
    for i in range(8):
        rows = pl.ds(i * 256, 256)
        for u in range(2):
            got = acc[u, rows, :] + tdot(colb_v[:, rows], dual[:, u * HALF:(u + 1) * HALF])
            if u:
                got = got + tdot(side_v[pl.ds(LEAF - LAST, LAST), rows], nbl[pl.ds(0, LAST), :])
            tmp[rows, u * HALF:(u + 1) * HALF] = got
        pltpu.make_async_copy(tmp.at[rows], out.at[rows], sem).start()
    pltpu.make_async_copy(tmp, out, sem).wait()


def on_device(*args):
    res, selft, sidet, rowb, colb, coup, side, targ, rank, count = args
    anyspace = pl.BlockSpec(memory_space=pl.ANY)
    vm = pl.BlockSpec(memory_space=pltpu.VMEM)
    hbm = pl.BlockSpec(memory_space=pltpu.HBM)
    dma = pltpu.SemaphoreType.DMA
    n = len(PIECES)
    ins = (
        res[0, 0], selft[0, 0], sidet[0, 0], rowb[0, 0].T, colb[0, 0].T,
        coup[0, 0].transpose(1, 2, 0).reshape(K * K, ADM), targ[0], rank[0], side, count,
    )
    ins = [a if a.size == 1 else pltpu.with_memory_space_constraint(a, pltpu.HBM) for a in ins]
    mid = pl.pallas_call(
        kernel,
        out_shape=[
            pltpu.VMEM((2, LEAF, HALF), F32), pltpu.VMEM((LEAF, LEAF), BF), pltpu.VMEM((512, HALF), BF),
            pltpu.VMEM((K, LEAF), BF), pltpu.VMEM((K, NRHS), BF),
        ],
        in_specs=[hbm] * 8 + [anyspace] * 2,
        out_specs=[vm] * 5,
        scratch_shapes=[
            pltpu.VMEM((2, LEAF, HALF), BF),
            pltpu.VMEM((LEAF, LEAF), BF),
            pltpu.VMEM((K, LEAF), BF),
            pltpu.VMEM((K * K, ADM), BF),
            pltpu.VMEM((1, ADM), jnp.int32),
            pltpu.VMEM((1, ADM), jnp.int32),
            pltpu.VMEM((1, 1), jnp.int32),
            pltpu.VMEM((1, 1), jnp.int32),
            pltpu.VMEM((2, LEAF, HALF), BF),
            pltpu.VMEM((2, LEAF, HALF), BF),
            pltpu.VMEM((1, ADM), jnp.int32),
            pltpu.VMEM((512, 128), BF),
            pltpu.VMEM((512, 128), BF),
            pltpu.VMEM((4, 8 * K, 128), F32),
            pltpu.VMEM((2, 8, K, 128), BF),
            pltpu.VMEM((2, 8, K, 384), BF),
            pltpu.VMEM((16, K, 128), BF),
            pltpu.VMEM((16, K, 384), BF),
            pltpu.VMEM((16, K, NRHS), BF),
            pltpu.VMEM((3, 128, NRHS), F32),
            pltpu.VMEM((2, 128, HALF), BF),
            pltpu.VMEM((2, 128, NRHS), BF),
            pltpu.VMEM((2, 128, HALF), BF),
            pltpu.VMEM((2, 128, NRHS), BF),
            pltpu.VMEM((4, K, NRHS), BF),
            pltpu.VMEM((K, NRHS), BF),
            pltpu.VMEM((K, NRHS), BF),
            dma((10,)), dma((10,)), dma((n,)), dma, dma, dma((3,)), dma((2,)), dma((2,)), dma((2,)), dma, dma, dma, dma,
        ],
        compiler_params=pltpu.CompilerParams(
            collective_id=0, has_side_effects=True, vmem_limit_bytes=36 * 2**20
        ),
    )(*ins)
    out = pl.pallas_call(
        finish,
        out_shape=jax.ShapeDtypeStruct((LEAF, NRHS), F32),
        in_specs=[vm] * 5,
        out_specs=anyspace,
        scratch_shapes=[pltpu.VMEM((LEAF, NRHS), F32), dma],
        compiler_params=pltpu.CompilerParams(vmem_limit_bytes=12 * 2**20),
    )(*mid)
    return out[None, None]


def solution(mesh):
    rc = ("row", "col")
    in_specs = tuple(P(*rc, *[None] * n) for n in (2, 2, 2, 2, 2, 3, 0, 1, 1, 0))
    return jax.shard_map(
        on_device, mesh=mesh, in_specs=in_specs, out_specs=P(*rc, None, None), check_vma=False
    )
```

```python
import jax
import jax.numpy as jnp
from jax import lax
from jax.experimental import pallas as pl
from jax.experimental.pallas import tpu as pltpu
from jax.sharding import PartitionSpec as P

MESH = pl.DeviceIdType.MESH
LEAF, K, NRHS, ADM = 2048, 32, 512, 64
HALF = NRHS // 2
BF, F32 = jnp.bfloat16, jnp.float32
PIECES = [(0, i * 512, 512) for i in range(4)] + [(1, i * 512, 512) for i in range(3)] + [(1, 1536, 288), (1, 1824, 224)]
LAST = 224


def tdot(a, b):
    return lax.dot_general(a, b, (((0,), (0,)), ((), ())), preferred_element_type=F32)


def scope(name):
    return jax.named_scope(name)


def kernel(
    res, selft, sidet, rowb, colb, coup, targ, rank, side, count,
    acc, side_v, nbl, colb_v, dual,
    res_v, self_v, rowb_v, coup_v, targ_v, rank_v, side_s, count_v, nb_on, nb_off,
    targ_r, raw_s, raw_r, d32, ds_a, ds_b, m_a, m_b, g_v, p32, p2, ps, q_v, r_v, qs, f_v, n_v,
    lsem, ssem, off_r, on_r, xp_r, w_r, z_r, c_r, m_r, q_r, y_r, f_r, n_r,
):
    p, q = lax.axis_index("row"), lax.axis_index("col")
    c, x, z = p % 2, (p // 2) % 4, q // 2
    y = (p // 8) * 2 + q % 2
    xp, h = x % 2, x // 2
    hx = 1 + h
    handler = x == hx
    near_core = hx % 2

    def dev(x_, y_, z_, c_):
        return ((y_ // 2) * 8 + x_ * 2 + c_, z_ * 2 + y_ % 2)

    off_dev = ((p + 15 + 2 * c) % 16, q)
    on_dev = (p + 1 - 2 * c, q)
    y_devs = [dev(x, (y + k) % 4, z, c) for k in (1, 2, 3)]
    side_x = 4 * h + 1 - x
    far_devs = [dev(2 - 2 * h + k // 2, y, z, k % 2) for k in range(4)]
    outer_dev = dev(hx, y, z, c)
    bar = pltpu.get_barrier_semaphore()
    common = [off_dev, dev(side_x, y, z, 0), dev(side_x, y, z, 1)]
    peers = [dev(x, y, (z + k % 4) % 4, (c + k // 4) % 2) for k in range(1, 8)]
    inner = common + far_devs + y_devs + peers
    outer = common + [on_dev] + [dev(2 - h, y, z, 0), dev(2 - h, y, z, 1)]

    @pl.when(handler)
    def _():
        for d in inner:
            pl.semaphore_signal(bar, 1, device_id=d, device_id_type=MESH)

    @pl.when(jnp.logical_not(handler))
    def _():
        for d in outer:
            pl.semaphore_signal(bar, 1, device_id=d, device_id_type=MESH)

    def load(k, src, dst):
        return pltpu.make_async_copy(src, dst, lsem.at[k])

    def done(ref, sem):
        pltpu.make_async_copy(ref, ref, sem).wait()

    small = [load(0, coup, coup_v), load(1, targ, targ_v), load(2, rank, rank_v), load(3, count, count_v), load(4, side, side_s)]
    load_rowb = load(5, rowb, rowb_v)
    first = [load_rowb, load(6, res.at[:, :HALF], res_v.at[0]), load(6, res.at[:, HALF:], res_v.at[1])]
    load_self, load_side, load_colb = load(7, selft, self_v), load(8, sidet, side_v), load(9, colb, colb_v)
    for cp in first + small + [load_self]:
        cp.start()

    with scope("A_wload"):
        for cp in small:
            cp.wait()
    r = lax.broadcasted_iota(jnp.int32, (K * K, ADM), 0)
    s_i = lax.broadcasted_iota(jnp.int32, (K * K, ADM), 1)
    live = (jnp.maximum(r // K, r % K) < rank_v[0:1, :]) & (s_i < count_v[0:1, 0:1])
    masked = jnp.where(live, coup_v[...].astype(F32), 0.0)
    raw_s[...] = jnp.concatenate([masked[:512], masked[512:]], axis=1).astype(BF)

    lane = lax.broadcasted_iota(jnp.int32, (8, 128), 1)

    def densify(raw, targets, slot, ready=None):
        r = lax.broadcasted_iota(jnp.int32, (256, 128), 0)
        at = lax.broadcasted_iota(jnp.int32, (256, 128), 1) // ADM == r // 128
        t, d = (r // 8) % 16, r % 8
        c2, z2 = d // 4, d % 4
        x3 = jnp.where(c2 == near_core, 2 * h, 2 - 2 * h) + (t // 2) % 2
        kk, ct = t // 4, t % 2
        y2 = (y + jnp.where(kk == 0, 2, jnp.where(kk == 1, 1, jnp.where(kk == 2, 3, 0)))) % 4
        j = ((y2 // 2) * 8 + x3 * 2 + ct) * 8 + z2 * 2 + y2 % 2
        row = targets[0:1, :]
        hit = jnp.where((jnp.concatenate([row, row], axis=1) == j) & at, 1.0, 0.0).astype(BF)

        def body(a, _):
            block = raw[pl.ds(pl.multiple_of(a * K, K), K), :]
            full = lax.dot_general(
                hit, jnp.concatenate([block] * 4, axis=0), (((1,), (1,)), ((), ())), preferred_element_type=F32
            )
            for v in range(2):
                for u in range(4):
                    got = jnp.zeros((8, 128), F32)
                    for i in range(4):
                        at = (16 * v + 4 * u + i) * 8
                        got = jnp.where(lane // K == i, full[at:at + 8, :], got)
                    d32[u, pl.ds(a + 16 * v, 8, stride=K), :] = got
            return 0

        lax.fori_loop(0, 8, body, 0, unroll=8)
        if ready is not None:
            ready()
        lax.fori_loop(8, 16, body, 0, unroll=8)
        ds_a[slot] = d32[0].reshape(8, K, 128).astype(BF)
        for u in range(3):
            ds_b[slot, :, :, u * 128:(u + 1) * 128] = d32[1 + u].reshape(8, K, 128).astype(BF)

    mine, mate = c * 8 + z, c * 8 + 4 + z
    me = jnp.where(handler, mine, mate)

    with scope("C_coef"):
        load_rowb.wait()
        done(res_v, lsem.at[6])
        for u in range(2):
            g_v[me, :, u * HALF:(u + 1) * HALF] = jnp.dot(
                rowb_v[...], res_v[u], preferred_element_type=F32
            ).astype(BF)

    def rdma(src, dst, s, r, d):
        return pltpu.make_async_remote_copy(
            src_ref=src, dst_ref=dst, send_sem=s, recv_sem=r, device_id=d, device_id_type=MESH
        )

    def off(k):
        u, r0, n = PIECES[k]
        rows = pl.ds(r0, n)
        return rdma(res_v.at[u, rows], nb_off.at[u, rows], ssem.at[0], off_r.at[k], off_dev)

    offs = [off(k) for k in range(len(PIECES))]
    on = rdma(res_v, nb_on, ssem.at[7], on_r, on_dev)
    xp_copy = rdma(g_v.at[me], g_v.at[me], ssem.at[8], xp_r, outer_dev)
    raw_copies = [
        rdma(raw_s.at[pl.ds(i * 256, 256)], raw_r.at[pl.ds(i * 256, 256)], ssem.at[1], w_r.at[i], outer_dev) for i in (0, 1)
    ]
    targ_copy = rdma(targ_v, targ_r, ssem.at[9], w_r.at[2], outer_dev)
    m_copies = []
    for i, src in enumerate((mine, mate)):
        for l, (ds, m) in enumerate(((ds_a, m_a), (ds_b, m_b))):
            m_copies.append([
                rdma(
                    ds.at[i, (c + k // 4) % 2 * 4 + (z + k) % 4], m.at[src], ssem.at[2], m_r.at[l],
                    dev(hx, y, (z + k) % 4, (c + k // 4) % 2),
                ) for k in range(1, 8)
            ])
    z_copies = [
        [
            rdma(g_v.at[src], g_v.at[src], ssem.at[3], z_r.at[i], dev(x, y, (z + k) % 4, c))
            for k in (2, 1, 3)
        ] for i, src in enumerate((mine, mate))
    ]
    c_copies = []
    for i in range(2):
        part = pl.ds(c * 8 + 4 * i, 4)
        c_copies.append(rdma(g_v.at[part], g_v.at[part], ssem.at[4], c_r.at[i], on_dev))

    with scope("D_bar"):
        @pl.when(handler)
        def _():
            pl.semaphore_wait(bar, len(inner))

        @pl.when(jnp.logical_not(handler))
        def _():
            pl.semaphore_wait(bar, len(outer))


    @pl.when(handler)
    def _():
        for cp in z_copies[0]:
            cp.start()

    @pl.when(jnp.logical_not(handler))
    def _():
        for cp in [targ_copy] + raw_copies + [xp_copy]:
            cp.start()

    for cp in offs:
        cp.start()
    on.start()
    load_side.start()
    load_colb.start()

    @pl.when(handler)
    def _():
        with scope("B_dense"):
            densify(raw_s, targ_v, 0)
        for cp in m_copies[0] + m_copies[1]:
            cp.start()
        m_a[mine] = ds_a[0, c * 4 + z]
        m_b[mine] = ds_b[0, c * 4 + z]

    def self_part(i, _):
        cols = pl.ds(pl.multiple_of(i * 256, 256), 256)
        got = tdot(self_v[:, cols], jnp.concatenate([res_v[0], res_v[1]], axis=1))
        acc[0, cols, :] = got[:, :HALF]
        acc[1, cols, :] = got[:, HALF:]
        return 0

    with scope("E_wself"):
        load_self.wait()
    q_copies = [rdma(p2.at[k], q_v.at[k], ssem.at[5], q_r, y_devs[2 * k]) for k in (0, 1)]
    y_copies = [rdma(ps.at[k], r_v.at[k], ssem.at[5], y_r, y_devs[2 * k]) for k in (0, 1)]
    near_is_me = c == near_core
    far = [rdma(qs.at[k], f_v, ssem.at[6], f_r, far_devs[k]) for k in range(4)]
    near = [rdma(qs.at[xp * 2 + 1 - c], n_v, ssem.at[6], n_r, on_dev)] + [
        rdma(qs.at[(1 - xp) * 2 + k], n_v, ssem.at[6], n_r, dev(side_x, y, z, k)) for k in (0, 1)
    ]

    with scope("E_self1"):
        self_part(0, 0)

    @pl.when(handler)
    def _():
        with scope("F_wraw"):
            targ_copy.wait_recv()
            raw_copies[0].wait_recv()
        with scope("F_dense"):
            densify(raw_r, targ_r, 1, raw_copies[1].wait_recv)
        for cp in m_copies[2]:
            cp.start()
        with scope("F_wxp"):
            xp_copy.wait_recv()
        for cp in z_copies[1] + m_copies[3]:
            cp.start()
        m_a[mate] = ds_a[1, c * 4 + z]
        m_b[mate] = ds_b[1, c * 4 + z]
        with scope("F_wz"):
            done(g_v.at[pl.ds(0, 3)], z_r.at[0])
        c_copies[0].start()

    with scope("F_self2"):
        lax.fori_loop(1, 7, self_part, 0, unroll=6)

    @pl.when(handler)
    def _():
        with scope("H_wz"):
            done(g_v.at[pl.ds(0, 3)], z_r.at[1])
        c_copies[1].start()

    with scope("H_self3"):
        self_part(7, 0)

    @pl.when(handler)
    def _():
        with scope("I_wma"):
            done(m_a.at[pl.ds(0, 14)], m_r.at[0])
        with scope("I_wc"):
            for cp in c_copies:
                cp.wait_recv()
        with scope("I_pa"):
            got = tdot(m_a[...].reshape(512, 128), g_v[...].reshape(512, NRHS)).astype(BF)
            p2[0] = got[:, :HALF]
            p2[1] = got[:, HALF:]
        for cp in q_copies:
            cp.start()
        with scope("I_wmb"):
            done(m_b.at[pl.ds(0, 14)], m_r.at[1])
        with scope("I_pb"):
            p32[...] = tdot(m_b[...].reshape(512, 384), g_v[...].reshape(512, NRHS)).reshape(3, 128, NRHS)

    which = side_s[0:1, 0:1]
    w_on = jnp.broadcast_to(jnp.where(which == 1 - 2 * c, 1.0, 0.0), (1, HALF)).astype(BF)
    w_off = jnp.broadcast_to(jnp.where(which == 2 * c - 1, 1.0, 0.0), (1, HALF)).astype(BF)
    with scope("G_won"):
        on.wait_recv()
        load_side.wait()

    def picked(k):
        u, r0, n = PIECES[k]
        rows = pl.ds(r0, n)
        with scope(f"w{k}"):
            offs[k].wait_recv()
        return nb_on[u, rows, :] * w_on + nb_off[u, rows, :] * w_off

    def side_part(k):
        u, r0, n = PIECES[k]
        nbl[pl.ds(0, n), :] = picked(k)
        with scope(f"S{k}"):
            def body(i, _):
                cols = pl.ds(pl.multiple_of(i * 512, 512), 512)
                acc[u, cols, :] += tdot(side_v[pl.ds(r0, n), cols], nbl[pl.ds(0, n), :])
                return 0

            lax.fori_loop(0, 4, body, 0, unroll=4)

    side_part(0)
    side_part(1)

    @pl.when(handler)
    def _():
        with scope("J_wq"):
            done(q_v, q_r)
        for k in range(2):
            cols = slice(k * HALF, (k + 1) * HALF)
            rest = slice((1 - k) * HALF, (2 - k) * HALF)
            ps[k, :, cols] = (p32[k, :, cols] + q_v[k].astype(F32)).astype(BF)
            ps[k, :, rest] = p32[k, :, rest].astype(BF)
            y_copies[k].start()

    side_part(2)
    side_part(3)

    @pl.when(handler)
    def _():
        with scope("K_wy"):
            done(r_v, y_r)
        total = p32[2] + r_v[0].astype(F32) + r_v[1].astype(F32)
        qs[...] = total.astype(BF).reshape(4, K, NRHS)

        @pl.when(near_is_me)
        def _():
            for cp in near:
                cp.start()
            n_v[...] = qs[xp * 2 + c]

        @pl.when(jnp.logical_not(near_is_me))
        def _():
            for cp in far:
                cp.start()

    side_part(4)
    side_part(5)
    side_part(6)
    side_part(7)
    with scope("Q_sends"):
        done(res_v, ssem.at[0])
        on.wait_send()

        @pl.when(handler)
        def _():
            done(g_v.at[pl.ds(0, 14)], ssem.at[2])
            done(g_v.at[pl.ds(0, 6)], ssem.at[3])
            done(g_v.at[pl.ds(0, 8)], ssem.at[4])
            done(g_v.at[pl.ds(0, 12)], ssem.at[5])

            @pl.when(near_is_me)
            def _():
                done(g_v.at[pl.ds(0, 3)], ssem.at[6])

            @pl.when(jnp.logical_not(near_is_me))
            def _():
                done(g_v.at[pl.ds(0, 4)], ssem.at[6])

        @pl.when(jnp.logical_not(handler))
        def _():
            done(raw_s, ssem.at[1])
            xp_copy.wait_send()
            targ_copy.wait_send()

    nbl[pl.ds(0, LAST), :] = picked(8)
    with scope("M_wfar"):
        far[0].wait_recv()

    with scope("M_wdual"):
        @pl.when(jnp.logical_not(handler & near_is_me))
        def _():
            near[0].wait_recv()

    load_colb.wait()
    dual[...] = (n_v[...].astype(F32) + f_v[...].astype(F32)).astype(BF)


def finish(acc, side_v, nbl, colb_v, dual, out, tmp, sem):
    right = jnp.concatenate([nbl[pl.ds(0, LAST), :], dual[:, HALF:]], axis=0)
    for i in range(8):
        rows = pl.ds(i * 256, 256)
        tmp[rows, :HALF] = acc[0, rows, :] + tdot(colb_v[:, rows], dual[:, :HALF])
        left = jnp.concatenate([side_v[pl.ds(LEAF - LAST, LAST), rows], colb_v[:, rows]], axis=0)
        tmp[rows, HALF:] = acc[1, rows, :] + tdot(left, right)
        pltpu.make_async_copy(tmp.at[rows], out.at[rows], sem).start()
    with scope("Z_wout"):
        pltpu.make_async_copy(tmp, out, sem).wait()


def on_device(*args):
    res, selft, sidet, rowb, colb, coup, side, targ, rank, count = args
    anyspace = pl.BlockSpec(memory_space=pl.ANY)
    vm = pl.BlockSpec(memory_space=pltpu.VMEM)
    hbm = pl.BlockSpec(memory_space=pltpu.HBM)
    dma = pltpu.SemaphoreType.DMA
    n = len(PIECES)
    ins = (
        res[0, 0], selft[0, 0], sidet[0, 0], rowb[0, 0].T, colb[0, 0].T,
        coup[0, 0].transpose(1, 2, 0).reshape(K * K, ADM), targ[0], rank[0], side, count,
    )
    ins = [a if a.size == 1 else pltpu.with_memory_space_constraint(a, pltpu.HBM) for a in ins]
    mid = pl.pallas_call(
        kernel,
        out_shape=[
            pltpu.VMEM((2, LEAF, HALF), F32), pltpu.VMEM((LEAF, LEAF), BF), pltpu.VMEM((512, HALF), BF),
            pltpu.VMEM((K, LEAF), BF), pltpu.VMEM((K, NRHS), BF),
        ],
        in_specs=[hbm] * 8 + [anyspace] * 2,
        out_specs=[vm] * 5,
        scratch_shapes=[
            pltpu.VMEM((2, LEAF, HALF), BF),
            pltpu.VMEM((LEAF, LEAF), BF),
            pltpu.VMEM((K, LEAF), BF),
            pltpu.VMEM((K * K, ADM), BF),
            pltpu.VMEM((1, ADM), jnp.int32),
            pltpu.VMEM((1, ADM), jnp.int32),
            pltpu.VMEM((1, 1), jnp.int32),
            pltpu.VMEM((1, 1), jnp.int32),
            pltpu.VMEM((2, LEAF, HALF), BF),
            pltpu.VMEM((2, LEAF, HALF), BF),
            pltpu.VMEM((1, ADM), jnp.int32),
            pltpu.VMEM((512, 128), BF),
            pltpu.VMEM((512, 128), BF),
            pltpu.VMEM((4, 8 * K, 128), F32),
            pltpu.VMEM((2, 8, K, 128), BF),
            pltpu.VMEM((2, 8, K, 384), BF),
            pltpu.VMEM((16, K, 128), BF),
            pltpu.VMEM((16, K, 384), BF),
            pltpu.VMEM((16, K, NRHS), BF),
            pltpu.VMEM((3, 128, NRHS), F32),
            pltpu.VMEM((2, 128, HALF), BF),
            pltpu.VMEM((2, 128, NRHS), BF),
            pltpu.VMEM((2, 128, HALF), BF),
            pltpu.VMEM((2, 128, NRHS), BF),
            pltpu.VMEM((4, K, NRHS), BF),
            pltpu.VMEM((K, NRHS), BF),
            pltpu.VMEM((K, NRHS), BF),
            dma((10,)), dma((10,)), dma((n,)), dma, dma, dma((3,)), dma((2,)), dma((2,)), dma((2,)), dma, dma, dma, dma,
        ],
        compiler_params=pltpu.CompilerParams(
            collective_id=0, has_side_effects=True, vmem_limit_bytes=36 * 2**20
        ),
    )(*ins)
    out = pl.pallas_call(
        finish,
        out_shape=jax.ShapeDtypeStruct((LEAF, NRHS), F32),
        in_specs=[vm] * 5,
        out_specs=anyspace,
        scratch_shapes=[pltpu.VMEM((LEAF, NRHS), F32), dma],
        compiler_params=pltpu.CompilerParams(vmem_limit_bytes=12 * 2**20),
    )(*mid)
    return out[None, None]


def solution(mesh):
    rc = ("row", "col")
    in_specs = tuple(P(*rc, *[None] * n) for n in (2, 2, 2, 2, 2, 3, 0, 1, 1, 0))
    return jax.shard_map(
        on_device, mesh=mesh, in_specs=in_specs, out_specs=P(*rc, None, None), check_vma=False
    )
```

```python
import jax
import jax.numpy as jnp
from jax import lax
from jax.experimental import pallas as pl
from jax.experimental.pallas import tpu as pltpu
from jax.sharding import PartitionSpec as P

MESH = pl.DeviceIdType.MESH
LEAF, K, NRHS, ADM = 2048, 32, 512, 64
HALF = NRHS // 2
BF, F32 = jnp.bfloat16, jnp.float32
PIECES = [(0, i * 512, 512) for i in range(4)] + [(1, i * 512, 512) for i in range(3)] + [(1, 1536, 288), (1, 1824, 224)]
LAST = 224


def tdot(a, b):
    return lax.dot_general(a, b, (((0,), (0,)), ((), ())), preferred_element_type=F32)


def scope(name):
    return jax.named_scope(name)


def kernel(
    res, selft, sidet, rowb, colb, coup, targ, rank, side, count,
    acc, side_v, nbl, colb_v, dual,
    res_v, self_v, rowb_v, coup_v, targ_v, rank_v, side_s, count_v, nb_on, nb_off,
    targ_r, raw_s, raw_r, d32, ds_a, ds_b, m_a, m_b, g_v, p32, p2, ps, q_v, r_v, qs, f_v, n_v,
    lsem, ssem, off_r, on_r, xp_r, w_r, z_r, c_r, m_r, q_r, y_r, f_r, n_r,
):
    p, q = lax.axis_index("row"), lax.axis_index("col")
    c, x, z = p % 2, (p // 2) % 4, q // 2
    y = (p // 8) * 2 + q % 2
    xp, h = x % 2, x // 2
    hx = 1 + h
    handler = x == hx
    near_core = hx % 2

    def dev(x_, y_, z_, c_):
        return ((y_ // 2) * 8 + x_ * 2 + c_, z_ * 2 + y_ % 2)

    off_dev = ((p + 15 + 2 * c) % 16, q)
    on_dev = (p + 1 - 2 * c, q)
    y_devs = [dev(x, (y + k) % 4, z, c) for k in (1, 2, 3)]
    side_x = 4 * h + 1 - x
    far_devs = [dev(2 - 2 * h + k // 2, y, z, k % 2) for k in range(4)]
    outer_dev = dev(hx, y, z, c)
    bar = pltpu.get_barrier_semaphore()
    common = [off_dev, dev(side_x, y, z, 0), dev(side_x, y, z, 1)]
    peers = [dev(x, y, (z + k % 4) % 4, (c + k // 4) % 2) for k in range(1, 8)]
    inner = common + far_devs + y_devs + peers
    outer = common + [on_dev] + [dev(2 - h, y, z, 0), dev(2 - h, y, z, 1)]

    @pl.when(handler)
    def _():
        for d in inner:
            pl.semaphore_signal(bar, 1, device_id=d, device_id_type=MESH)

    @pl.when(jnp.logical_not(handler))
    def _():
        for d in outer:
            pl.semaphore_signal(bar, 1, device_id=d, device_id_type=MESH)

    def load(k, src, dst):
        return pltpu.make_async_copy(src, dst, lsem.at[k])

    def done(ref, sem):
        pltpu.make_async_copy(ref, ref, sem).wait()

    small = [load(0, coup, coup_v), load(1, targ, targ_v), load(2, rank, rank_v), load(3, count, count_v), load(4, side, side_s)]
    load_rowb = load(5, rowb, rowb_v)
    first = [load_rowb, load(6, res.at[:, :HALF], res_v.at[0]), load(6, res.at[:, HALF:], res_v.at[1])]
    load_self, load_side, load_colb = load(7, selft, self_v), load(8, sidet, side_v), load(9, colb, colb_v)
    for cp in first + small + [load_self]:
        cp.start()

    with scope("A_wload"):
        for cp in small:
            cp.wait()
    r = lax.broadcasted_iota(jnp.int32, (K * K, ADM), 0)
    s_i = lax.broadcasted_iota(jnp.int32, (K * K, ADM), 1)
    live = (jnp.maximum(r // K, r % K) < rank_v[0:1, :]) & (s_i < count_v[0:1, 0:1])
    masked = jnp.where(live, coup_v[...].astype(F32), 0.0)
    raw_s[...] = jnp.concatenate([masked[:512], masked[512:]], axis=1).astype(BF)

    lane = lax.broadcasted_iota(jnp.int32, (8, 128), 1)

    def densify(raw, targets, slot, ready=None):
        r = lax.broadcasted_iota(jnp.int32, (256, 128), 0)
        at = lax.broadcasted_iota(jnp.int32, (256, 128), 1) // ADM == r // 128
        t, d = (r // 8) % 16, r % 8
        c2, z2 = d // 4, d % 4
        x3 = jnp.where(c2 == near_core, 2 * h, 2 - 2 * h) + (t // 2) % 2
        kk, ct = t // 4, t % 2
        y2 = (y + jnp.where(kk == 0, 2, jnp.where(kk == 1, 1, jnp.where(kk == 2, 3, 0)))) % 4
        j = ((y2 // 2) * 8 + x3 * 2 + ct) * 8 + z2 * 2 + y2 % 2
        row = targets[0:1, :]
        hit = jnp.where((jnp.concatenate([row, row], axis=1) == j) & at, 1.0, 0.0).astype(BF)

        def body(a, _):
            block = raw[pl.ds(pl.multiple_of(a * K, K), K), :]
            full = lax.dot_general(
                hit, jnp.concatenate([block] * 4, axis=0), (((1,), (1,)), ((), ())), preferred_element_type=F32
            )
            for v in range(2):
                for u in range(4):
                    got = jnp.zeros((8, 128), F32)
                    for i in range(4):
                        at = (16 * v + 4 * u + i) * 8
                        got = jnp.where(lane // K == i, full[at:at + 8, :], got)
                    d32[u, pl.ds(a + 16 * v, 8, stride=K), :] = got
            return 0

        lax.fori_loop(0, 8, body, 0, unroll=8)
        if ready is not None:
            ready()
        lax.fori_loop(8, 16, body, 0, unroll=8)
        ds_a[slot] = d32[0].reshape(8, K, 128).astype(BF)
        for u in range(3):
            ds_b[slot, :, :, u * 128:(u + 1) * 128] = d32[1 + u].reshape(8, K, 128).astype(BF)

    mine, mate = c * 8 + z, c * 8 + 4 + z
    me = jnp.where(handler, mine, mate)

    with scope("C_coef"):
        load_rowb.wait()
        done(res_v, lsem.at[6])
        for u in range(2):
            g_v[me, :, u * HALF:(u + 1) * HALF] = jnp.dot(
                rowb_v[...], res_v[u], preferred_element_type=F32
            ).astype(BF)

    def rdma(src, dst, s, r, d):
        return pltpu.make_async_remote_copy(
            src_ref=src, dst_ref=dst, send_sem=s, recv_sem=r, device_id=d, device_id_type=MESH
        )

    def off(k):
        u, r0, n = PIECES[k]
        rows = pl.ds(r0, n)
        return rdma(res_v.at[u, rows], nb_off.at[u, rows], ssem.at[0], off_r.at[k], off_dev)

    offs = [off(k) for k in range(len(PIECES))]
    on = rdma(res_v, nb_on, ssem.at[7], on_r, on_dev)
    xp_copy = rdma(g_v.at[me], g_v.at[me], ssem.at[8], xp_r, outer_dev)
    raw_copies = [
        rdma(raw_s.at[pl.ds(i * 256, 256)], raw_r.at[pl.ds(i * 256, 256)], ssem.at[1], w_r.at[i], outer_dev) for i in (0, 1)
    ]
    targ_copy = rdma(targ_v, targ_r, ssem.at[9], w_r.at[2], outer_dev)
    m_copies = []
    for i, src in enumerate((mine, mate)):
        for l, (ds, m) in enumerate(((ds_a, m_a), (ds_b, m_b))):
            m_copies.append([
                rdma(
                    ds.at[i, (c + k // 4) % 2 * 4 + (z + k) % 4], m.at[src], ssem.at[2], m_r.at[l],
                    dev(hx, y, (z + k) % 4, (c + k // 4) % 2),
                ) for k in range(1, 8)
            ])
    z_copies = [
        [
            rdma(g_v.at[src], g_v.at[src], ssem.at[3], z_r.at[i], dev(x, y, (z + k) % 4, c))
            for k in (2, 1, 3)
        ] for i, src in enumerate((mine, mate))
    ]
    c_copies = []
    for i in range(2):
        part = pl.ds(c * 8 + 4 * i, 4)
        c_copies.append(rdma(g_v.at[part], g_v.at[part], ssem.at[4], c_r.at[i], on_dev))

    with scope("D_bar"):
        @pl.when(handler)
        def _():
            pl.semaphore_wait(bar, len(inner))

        @pl.when(jnp.logical_not(handler))
        def _():
            pl.semaphore_wait(bar, len(outer))


    @pl.when(handler)
    def _():
        for cp in z_copies[0]:
            cp.start()

    @pl.when(jnp.logical_not(handler))
    def _():
        for cp in [xp_copy, targ_copy] + raw_copies:
            cp.start()

    for cp in offs[:8]:
        cp.start()

    @pl.when(jnp.logical_not(handler))
    def _():
        for cp in offs[8:]:
            cp.start()

    on.start()
    load_side.start()
    load_colb.start()

    @pl.when(handler)
    def _():
        with scope("B_dense"):
            densify(raw_s, targ_v, 0)
        for cp in m_copies[0] + m_copies[1]:
            cp.start()
        m_a[mine] = ds_a[0, c * 4 + z]
        m_b[mine] = ds_b[0, c * 4 + z]

    def self_part(i, _):
        cols = pl.ds(pl.multiple_of(i * 256, 256), 256)
        got = tdot(self_v[:, cols], jnp.concatenate([res_v[0], res_v[1]], axis=1))
        acc[0, cols, :] = got[:, :HALF]
        acc[1, cols, :] = got[:, HALF:]
        return 0

    with scope("E_wself"):
        load_self.wait()
    q_copies = [rdma(p2.at[k], q_v.at[k], ssem.at[5], q_r, y_devs[2 * k]) for k in (0, 1)]
    y_copies = [rdma(ps.at[k], r_v.at[k], ssem.at[5], y_r, y_devs[2 * k]) for k in (0, 1)]
    near_is_me = c == near_core
    far = [rdma(qs.at[k], f_v, ssem.at[6], f_r, far_devs[k]) for k in range(4)]
    near = [rdma(qs.at[xp * 2 + 1 - c], n_v, ssem.at[6], n_r, on_dev)] + [
        rdma(qs.at[(1 - xp) * 2 + k], n_v, ssem.at[6], n_r, dev(side_x, y, z, k)) for k in (0, 1)
    ]

    with scope("E_self1"):
        self_part(0, 0)

    @pl.when(handler)
    def _():
        with scope("F_wxp"):
            xp_copy.wait_recv()
        for cp in z_copies[1]:
            cp.start()
        with scope("F_wraw"):
            targ_copy.wait_recv()
            raw_copies[0].wait_recv()
        with scope("F_dense"):
            densify(raw_r, targ_r, 1, raw_copies[1].wait_recv)
        for cp in m_copies[2]:
            cp.start()
        m_a[mate] = ds_a[1, c * 4 + z]
        m_b[mate] = ds_b[1, c * 4 + z]
        with scope("F_wz"):
            done(g_v.at[pl.ds(0, 3)], z_r.at[0])
        c_copies[0].start()

    with scope("F_self2"):
        lax.fori_loop(1, 4, self_part, 0, unroll=3)

    @pl.when(handler)
    def _():
        for cp in m_copies[3]:
            cp.start()

    with scope("F_self3"):
        lax.fori_loop(4, 7, self_part, 0, unroll=3)

    @pl.when(handler)
    def _():
        with scope("H_wz"):
            done(g_v.at[pl.ds(0, 3)], z_r.at[1])
        c_copies[1].start()

    with scope("H_self3"):
        self_part(7, 0)

    @pl.when(handler)
    def _():
        with scope("I_wma"):
            done(m_a.at[pl.ds(0, 14)], m_r.at[0])
        with scope("I_wc"):
            for cp in c_copies:
                cp.wait_recv()
        with scope("I_pa"):
            got = tdot(m_a[...].reshape(512, 128), g_v[...].reshape(512, NRHS)).astype(BF)
            p2[0] = got[:, :HALF]
            p2[1] = got[:, HALF:]
        for cp in q_copies:
            cp.start()
        with scope("I_wmb"):
            done(m_b.at[pl.ds(0, 14)], m_r.at[1])
        with scope("I_pb"):
            p32[...] = tdot(m_b[...].reshape(512, 384), g_v[...].reshape(512, NRHS)).reshape(3, 128, NRHS)

    which = side_s[0:1, 0:1]
    w_on = jnp.broadcast_to(jnp.where(which == 1 - 2 * c, 1.0, 0.0), (1, HALF)).astype(BF)
    w_off = jnp.broadcast_to(jnp.where(which == 2 * c - 1, 1.0, 0.0), (1, HALF)).astype(BF)
    with scope("G_won"):
        on.wait_recv()
        load_side.wait()

    def picked(k):
        u, r0, n = PIECES[k]
        rows = pl.ds(r0, n)
        with scope(f"w{k}"):
            offs[k].wait_recv()
        return nb_on[u, rows, :] * w_on + nb_off[u, rows, :] * w_off

    def side_part(k):
        u, r0, n = PIECES[k]
        nbl[pl.ds(0, n), :] = picked(k)
        with scope(f"S{k}"):
            def body(i, _):
                cols = pl.ds(pl.multiple_of(i * 512, 512), 512)
                acc[u, cols, :] += tdot(side_v[pl.ds(r0, n), cols], nbl[pl.ds(0, n), :])
                return 0

            lax.fori_loop(0, 4, body, 0, unroll=4)

    side_part(0)
    side_part(1)

    @pl.when(handler)
    def _():
        with scope("J_wq"):
            done(q_v, q_r)
        for k in range(2):
            cols = slice(k * HALF, (k + 1) * HALF)
            rest = slice((1 - k) * HALF, (2 - k) * HALF)
            ps[k, :, cols] = (p32[k, :, cols] + q_v[k].astype(F32)).astype(BF)
            ps[k, :, rest] = p32[k, :, rest].astype(BF)
            y_copies[k].start()

    side_part(2)
    side_part(3)

    @pl.when(handler)
    def _():
        with scope("K_wy"):
            done(r_v, y_r)
        total = p32[2] + r_v[0].astype(F32) + r_v[1].astype(F32)
        qs[...] = total.astype(BF).reshape(4, K, NRHS)

        @pl.when(near_is_me)
        def _():
            for cp in near:
                cp.start()
            n_v[...] = qs[xp * 2 + c]

        @pl.when(jnp.logical_not(near_is_me))
        def _():
            for cp in far:
                cp.start()

        for cp in offs[8:]:
            cp.start()

    side_part(4)
    side_part(5)
    side_part(6)
    side_part(7)
    with scope("Q_sends"):
        done(res_v, ssem.at[0])
        on.wait_send()

        @pl.when(handler)
        def _():
            done(g_v.at[pl.ds(0, 14)], ssem.at[2])
            done(g_v.at[pl.ds(0, 6)], ssem.at[3])
            done(g_v.at[pl.ds(0, 8)], ssem.at[4])
            done(g_v.at[pl.ds(0, 12)], ssem.at[5])

            @pl.when(near_is_me)
            def _():
                done(g_v.at[pl.ds(0, 3)], ssem.at[6])

            @pl.when(jnp.logical_not(near_is_me))
            def _():
                done(g_v.at[pl.ds(0, 4)], ssem.at[6])

        @pl.when(jnp.logical_not(handler))
        def _():
            done(raw_s, ssem.at[1])
            xp_copy.wait_send()
            targ_copy.wait_send()

    nbl[pl.ds(0, LAST), :] = picked(8)
    with scope("M_wfar"):
        far[0].wait_recv()

    with scope("M_wdual"):
        @pl.when(jnp.logical_not(handler & near_is_me))
        def _():
            near[0].wait_recv()

    load_colb.wait()
    dual[...] = (n_v[...].astype(F32) + f_v[...].astype(F32)).astype(BF)


def finish(acc, side_v, nbl, colb_v, dual, out, tmp, sem):
    right = jnp.concatenate([nbl[pl.ds(0, LAST), :], dual[:, HALF:]], axis=0)
    for i in range(8):
        rows = pl.ds(i * 256, 256)
        tmp[rows, :HALF] = acc[0, rows, :] + tdot(colb_v[:, rows], dual[:, :HALF])
        left = jnp.concatenate([side_v[pl.ds(LEAF - LAST, LAST), rows], colb_v[:, rows]], axis=0)
        tmp[rows, HALF:] = acc[1, rows, :] + tdot(left, right)
        pltpu.make_async_copy(tmp.at[rows], out.at[rows], sem).start()
    with scope("Z_wout"):
        pltpu.make_async_copy(tmp, out, sem).wait()


def on_device(*args):
    res, selft, sidet, rowb, colb, coup, side, targ, rank, count = args
    anyspace = pl.BlockSpec(memory_space=pl.ANY)
    vm = pl.BlockSpec(memory_space=pltpu.VMEM)
    hbm = pl.BlockSpec(memory_space=pltpu.HBM)
    dma = pltpu.SemaphoreType.DMA
    n = len(PIECES)
    ins = (
        res[0, 0], selft[0, 0], sidet[0, 0], rowb[0, 0].T, colb[0, 0].T,
        coup[0, 0].transpose(1, 2, 0).reshape(K * K, ADM), targ[0], rank[0], side, count,
    )
    ins = [a if a.size == 1 else pltpu.with_memory_space_constraint(a, pltpu.HBM) for a in ins]
    mid = pl.pallas_call(
        kernel,
        out_shape=[
            pltpu.VMEM((2, LEAF, HALF), F32), pltpu.VMEM((LEAF, LEAF), BF), pltpu.VMEM((512, HALF), BF),
            pltpu.VMEM((K, LEAF), BF), pltpu.VMEM((K, NRHS), BF),
        ],
        in_specs=[hbm] * 8 + [anyspace] * 2,
        out_specs=[vm] * 5,
        scratch_shapes=[
            pltpu.VMEM((2, LEAF, HALF), BF),
            pltpu.VMEM((LEAF, LEAF), BF),
            pltpu.VMEM((K, LEAF), BF),
            pltpu.VMEM((K * K, ADM), BF),
            pltpu.VMEM((1, ADM), jnp.int32),
            pltpu.VMEM((1, ADM), jnp.int32),
            pltpu.VMEM((1, 1), jnp.int32),
            pltpu.VMEM((1, 1), jnp.int32),
            pltpu.VMEM((2, LEAF, HALF), BF),
            pltpu.VMEM((2, LEAF, HALF), BF),
            pltpu.VMEM((1, ADM), jnp.int32),
            pltpu.VMEM((512, 128), BF),
            pltpu.VMEM((512, 128), BF),
            pltpu.VMEM((4, 8 * K, 128), F32),
            pltpu.VMEM((2, 8, K, 128), BF),
            pltpu.VMEM((2, 8, K, 384), BF),
            pltpu.VMEM((16, K, 128), BF),
            pltpu.VMEM((16, K, 384), BF),
            pltpu.VMEM((16, K, NRHS), BF),
            pltpu.VMEM((3, 128, NRHS), F32),
            pltpu.VMEM((2, 128, HALF), BF),
            pltpu.VMEM((2, 128, NRHS), BF),
            pltpu.VMEM((2, 128, HALF), BF),
            pltpu.VMEM((2, 128, NRHS), BF),
            pltpu.VMEM((4, K, NRHS), BF),
            pltpu.VMEM((K, NRHS), BF),
            pltpu.VMEM((K, NRHS), BF),
            dma((10,)), dma((10,)), dma((n,)), dma, dma, dma((3,)), dma((2,)), dma((2,)), dma((2,)), dma, dma, dma, dma,
        ],
        compiler_params=pltpu.CompilerParams(
            collective_id=0, has_side_effects=True, vmem_limit_bytes=36 * 2**20
        ),
    )(*ins)
    out = pl.pallas_call(
        finish,
        out_shape=jax.ShapeDtypeStruct((LEAF, NRHS), F32),
        in_specs=[vm] * 5,
        out_specs=anyspace,
        scratch_shapes=[pltpu.VMEM((LEAF, NRHS), F32), dma],
        compiler_params=pltpu.CompilerParams(vmem_limit_bytes=12 * 2**20),
    )(*mid)
    return out[None, None]


def solution(mesh):
    rc = ("row", "col")
    in_specs = tuple(P(*rc, *[None] * n) for n in (2, 2, 2, 2, 2, 3, 0, 1, 1, 0))
    return jax.shard_map(
        on_device, mesh=mesh, in_specs=in_specs, out_specs=P(*rc, None, None), check_vma=False
    )
```
